32 devices in a mesh: lat: 2 (over x), lon: 2 (over y), lev: 8 (over z, core).
Axes of the slice: x: 2, y: 2, z: 4, core: 2. Of those that a mesh axis runs over, the one named last changes fastest.
Arguments:
- along_axis_flow: bfloat16 [80, 4, 32, 1440], P(('lat', 'lev'), None, None, 'lon'), may hold values from -6 to 6
- poleward_flow: bfloat16 [80, 4, 32, 1440], P(('lat', 'lev'), None, None, 'lon'), may hold values from -6 to 6
- warmth_departure: bfloat16 [80, 4, 32, 1440], P(('lat', 'lev'), None, None, 'lon'), may hold values from -6 to 6
- validity_indicator: int32 [80, 32, 1440], P(('lat', 'lev'), None, 'lon'), may hold values from 0 to 1
- layer_depth_span: float32 [32], replicated, may hold values from 0.3 to 3
- desired_circulation_norm: float32 [80, 4, 32], P(('lat', 'lev')), may hold values from -4 to 4
Outputs:
- psi_norm: float32 [80, 4, 32], P(('lat', 'lev'))
- heat_cospec: float32 [720, 80, 128], P('lon', ('lat', 'lev'))
- momentum_cospec: float32 [720, 80, 128], P('lon', ('lat', 'lev'))
- budget_penalty: float32 [], replicated
The draws below stay inside these ranges and needn't reach their ends.
All inputs are finite; a program needn't handle non-finite values. Where the reference program divides by a largest or mean magnitude, that divisor is 1e-20 or more.
Results may differ from the reference program's by a relative error of at most 0.0033.
Values may be sent and summed in bfloat16 or wider, within the bound.
A program may use at most 64 MiB of HBM per device.

```python
import math
import jax
import jax.numpy as jnp
from jax import lax

ENSEMBLE_MEMBERS = 4
ISOBARIC_SHEETS = 32
GRID_MERIDIANS = 1440
HARMONIC_ORDERS = 720
POLAR_ANGLES = 80


def draw_validity_indicator(key, part):
    first_key, second_key = jax.random.split(jax.random.fold_in(key, 11))
    row_rate = jax.random.randint(first_key, (POLAR_ANGLES, ISOBARIC_SHEETS, 1), 0, 9)
    cell_draw = jax.random.randint(second_key, (POLAR_ANGLES, ISOBARIC_SHEETS, GRID_MERIDIANS), 0, 8)
    return (cell_draw < row_rate).astype(jnp.int32)


def shard_levels(own_key, extent, cuts, least, largest):
    def one(position, shards_of):
        heights = jax.random.uniform(jax.random.fold_in(jax.random.fold_in(own_key, 6), position), (shards_of,), jnp.float32, least / len(cuts), largest / len(cuts))
        return jnp.repeat(jnp.exp(heights), extent[position] // shards_of).reshape((-1,) + (1,) * (len(extent) - position - 1))

    loudness = one(*cuts[0])
    for cut in cuts[1:]:
        loudness = loudness * one(*cut)
    return loudness


def centred(stream_key, extent, spread, reach, shards=(), held_as=jnp.bfloat16):
    result = jax.random.normal(stream_key, extent, jnp.float32) * spread
    if len(shards) > 0:
        result = shard_levels(stream_key, extent, shards, -0.22, 0.18) * result
    return jnp.clip(result, min=-reach, max=reach).astype(held_as)


def setup_inputs(seed: int = 0) -> dict:
    seeds = jax.random.split(jax.random.key(seed), 7)
    along_axis_flow = centred(seeds[0], (POLAR_ANGLES, ENSEMBLE_MEMBERS, ISOBARIC_SHEETS, GRID_MERIDIANS), 1.0, 6.0, ((0, 16), (3, 2)))
    poleward_flow = centred(seeds[1], (POLAR_ANGLES, ENSEMBLE_MEMBERS, ISOBARIC_SHEETS, GRID_MERIDIANS), 1.0, 6.0, ((0, 16), (3, 2)))
    warmth_departure = centred(seeds[2], (POLAR_ANGLES, ENSEMBLE_MEMBERS, ISOBARIC_SHEETS, GRID_MERIDIANS), 1.0, 6.0, ((0, 16), (3, 2)))
    validity_indicator = draw_validity_indicator(jax.random.fold_in(seeds[6], 71), 0)
    layer_depth_span = jnp.clip(jnp.exp(jax.random.uniform(seeds[4], (ISOBARIC_SHEETS,), jnp.float32, math.log(0.3), math.log(3.0))), 0.3, 3.0)
    desired_circulation_norm = centred(seeds[5], (POLAR_ANGLES, ENSEMBLE_MEMBERS, ISOBARIC_SHEETS), 0.5, 4.0, ((0, 16),), jnp.float32)
    return {"along_axis_flow": along_axis_flow, "poleward_flow": poleward_flow, "warmth_departure": warmth_departure, "validity_indicator": validity_indicator, "layer_depth_span": layer_depth_span, "desired_circulation_norm": desired_circulation_norm}


epsilon = 1e-6


def build_waves(wave_rows, lon_index):
    wavenumber = wave_rows // 2 + 1
    component = wave_rows % 2
    turns = (wavenumber[:, None] * lon_index[None, :]) % GRID_MERIDIANS
    angle = turns.astype(jnp.float32) * (2.0 * math.pi / GRID_MERIDIANS)
    return jnp.where(component[:, None] == 0, jnp.cos(angle), jnp.sin(angle)).astype(jnp.bfloat16)


def reference(along_axis_flow, poleward_flow, warmth_departure, validity_indicator, layer_depth_span, desired_circulation_norm):
    retained_indicator = validity_indicator.astype(jnp.bfloat16)
    waves_table = build_waves(jnp.arange(2 * HARMONIC_ORDERS, dtype=jnp.int32), jnp.arange(GRID_MERIDIANS, dtype=jnp.int32))
    norm_factor = 2.0 / (GRID_MERIDIANS * GRID_MERIDIANS)

    def one_circle_slice(items):
        u_row, v_row, t_row, keep_row = items
        input_tensors = jnp.stack([u_row * keep_row[None], v_row * keep_row[None], t_row * keep_row[None]])
        input_tensors = input_tensors.reshape(3, ENSEMBLE_MEMBERS * ISOBARIC_SHEETS, GRID_MERIDIANS)
        fourier_weights = lax.dot_general(waves_table, input_tensors, (((1,), (2,)), ((), ())), preferred_element_type=jnp.float32)
        fourier_weights = fourier_weights.reshape(HARMONIC_ORDERS, 2, 3, ENSEMBLE_MEMBERS * ISOBARIC_SHEETS)
        heat_part = norm_factor * (fourier_weights[:, 0, 1] * fourier_weights[:, 0, 2] + fourier_weights[:, 1, 1] * fourier_weights[:, 1, 2])
        moment_part = norm_factor * (fourier_weights[:, 0, 0] * fourier_weights[:, 0, 1] + fourier_weights[:, 1, 0] * fourier_weights[:, 1, 1])
        return heat_part, moment_part

    thermal_transport_sum, eastward_stress_sum = lax.map(one_circle_slice, (along_axis_flow, poleward_flow, warmth_departure, retained_indicator))
    heat_cospec = jnp.transpose(thermal_transport_sum, (1, 0, 2))
    momentum_cospec = jnp.transpose(eastward_stress_sum, (1, 0, 2))

    screened_northward_speed = poleward_flow * retained_indicator[:, None]
    zonal_v = jnp.sum(screened_northward_speed, axis=3, dtype=jnp.float32)
    kept_count = jnp.sum(validity_indicator, axis=2).astype(jnp.float32)
    mean_v = zonal_v / jnp.maximum(kept_count, 1.0)[:, None, :]
    rows_lat = jnp.arange(POLAR_ANGLES, dtype=jnp.int32).astype(jnp.float32)
    latitude = ((rows_lat + 0.5) / POLAR_ANGLES - 0.5) * math.pi
    cosine = jnp.cos(latitude)
    weighted = mean_v * cosine[:, None, None] * layer_depth_span[None, None, :]
    stream = jnp.cumsum(jnp.cumsum(weighted, axis=2), axis=0)
    peak_value = jnp.max(jnp.abs(stream))
    psi_norm = stream / (peak_value + epsilon)
    residual_accumulator = jnp.sum(cosine[:, None, None] * (psi_norm - desired_circulation_norm) ** 2)
    budget_penalty = residual_accumulator / (ENSEMBLE_MEMBERS * ISOBARIC_SHEETS * POLAR_ANGLES)
    return psi_norm, heat_cospec, momentum_cospec, budget_penalty
```

```python
import functools
import math

import jax
import jax.numpy as jnp
import numpy as np
from jax import lax
from jax.experimental import pallas as pl
from jax.experimental.pallas import tpu as pltpu
from jax.sharding import PartitionSpec as P

HARMONIC_ORDERS = 720
epsilon = 1e-06
F32 = jnp.float32
BF16 = jnp.bfloat16


def round_up(value, step):
    return -(-value // step) * step


def wave_table(meridians, parts, rows, padded, span):
    wavenumber = np.arange(1, HARMONIC_ORDERS + 1, dtype=np.int64)
    turns = (wavenumber[:, None] * np.arange(span)[None, :]) % meridians
    angle = turns.astype(np.float32) * np.float32(2.0 * math.pi / meridians)
    waves = np.stack([np.cos(angle), np.sin(angle)]).astype(np.float32)
    waves = waves.reshape(2, parts, rows, span).transpose(1, 0, 2, 3)
    table = np.zeros((parts, 2, padded, span), np.float32)
    table[:, :, :rows] = waves
    return table.astype(jnp.bfloat16)


def nt_dot(a, b):
    return lax.dot_general(a, b, (((1,), (1,)), ((), ())), preferred_element_type=F32)


def kernel(
    sizes,
    u_ref,
    v_ref,
    t_ref,
    keep_ref,
    table_ref,
    cosine_ref,
    depth_ref,
    target_ref,
    psi_ref,
    heat_ref,
    moment_ref,
    penalty_ref,
    raw,
    keep,
    masked,
    doubled,
    arrived,
    table,
    given,
    returned,
    zonal_mine,
    zonal_theirs,
    mean_mine,
    gathered,
    stream_buf,
    load_sem,
    table_sem,
    field_send,
    field_recv,
    back_send,
    back_recv,
    zonal_sem,
    mean_send,
    mean_recv,
):
    bands, batch, levels, span, rows, rows_sent, groups, lev_ways = sizes
    columns = batch * levels
    padded_rows = table.shape[2]
    half, mid = bands // 2, bands % 2
    half_columns = columns // 2
    slab = mean_mine.shape[0] // 2
    me = lax.axis_index("lon")
    other = 1 - me
    mine = lax.axis_index("lat") * lev_ways + lax.axis_index("lev")
    partner = {"lon": other}
    norm_factor = 2.0 / (4.0 * span * span)

    their_rows = [other * (half + mid) + i for i in range(half)]
    my_rows = [me * (half + mid) + i for i in range(half)]
    order = ([half] if mid else []) + their_rows + my_rows

    loads = []
    for place, row in enumerate(order):
        loads.append(
            [
                pltpu.make_async_copy(keep_ref.at[row], keep.at[row], load_sem.at[place, 3]),
                pltpu.make_async_copy(u_ref.at[row], raw.at[row, 0], load_sem.at[place, 0]),
                pltpu.make_async_copy(v_ref.at[row], raw.at[row, 1], load_sem.at[place, 1]),
                pltpu.make_async_copy(t_ref.at[row], raw.at[row, 2], load_sem.at[place, 2]),
            ]
        )
        for copy in loads[-1]:
            copy.start()
    table_load = pltpu.make_async_copy(table_ref, table, table_sem)
    table_load.start()

    def mask_row(place):
        row = order[place]
        for copy in loads[place]:
            copy.wait()
        ones = keep[row].astype(F32).astype(BF16)
        for field in range(3):
            for sample in range(batch):
                part = pl.ds(sample * levels, levels)
                masked[row, field, part, :] = raw[row, field, part, :] * ones

    def remote(src, dst, send, recv):
        return pltpu.make_async_remote_copy(
            src_ref=src,
            dst_ref=dst,
            send_sem=send,
            recv_sem=recv,
            device_id=partner,
            device_id_type=pl.DeviceIdType.MESH,
        )

    field_copies = []

    def send_row(piece, place):
        row = order[place]
        if mid and piece == 0:
            away = pl.ds(pl.multiple_of(other * half_columns, half_columns), half_columns)
            copies = [
                remote(
                    masked.at[row, field, away, :],
                    arrived.at[piece, field, pl.ds(0, half_columns), :],
                    field_send.at[piece, field],
                    field_recv.at[piece, field],
                )
                for field in range(3)
            ]
        else:
            copies = [
                remote(
                    masked.at[row, field],
                    arrived.at[piece, field],
                    field_send.at[piece, field],
                    field_recv.at[piece, field],
                )
                for field in range(3)
            ]
        for copy in copies:
            copy.start()
        field_copies.append(copies)

    early = min(mid + 1, mid + half)
    for place in range(early):
        mask_row(place)
        send_row(place, place)
    for place in range(early, len(order)):
        mask_row(place)

    ones_row = jnp.ones((8, span), BF16)
    zonal_mine[...] = jnp.zeros_like(zonal_mine)
    for row in range(bands):
        zonal_mine[pl.ds(row, 1), :] = nt_dot(ones_row, masked[row, 1])[0:1]
        counts = nt_dot(ones_row, keep[row].astype(F32).astype(BF16))[0:1]
        zonal_mine[pl.ds(slab + row, 1), :] = jnp.concatenate([counts] * batch, axis=1)
    zonal_copy = remote(zonal_mine, zonal_theirs, zonal_sem.at[0], zonal_sem.at[1])
    zonal_copy.start()
    for place in range(early, mid + half):
        send_row(place, place)

    if mid:
        here = pl.ds(pl.multiple_of(me * half_columns, half_columns), half_columns)
        for field in range(3):
            own = masked[half, field, here, :]
            doubled[field, pl.ds(0, half_columns), :] = own
            doubled[field, pl.ds(half_columns, half_columns), :] = own
    table_load.wait()

    row_index = lax.broadcasted_iota(jnp.int32, (padded_rows, 1), 0)
    left_lanes = lax.broadcasted_iota(jnp.int32, (1, columns), 1) < half_columns
    back_copies = []

    def transform(part, near, far):
        parity = (row_index + 1 + part * rows) % 2
        sign = (1 - 2 * parity).astype(F32)
        pieces = []
        for trig in range(2):
            wave = table[part, trig]
            pieces.append([nt_dot(wave, near(f)) + sign * nt_dot(wave, far(f)) for f in range(3)])
        (uc, vc, tc), (us, vs, ts) = pieces
        return norm_factor * (vc * tc + vs * ts), norm_factor * (uc * vc + us * vs)

    def process(piece):
        for copy in field_copies[piece]:
            copy.wait_recv()
        is_mid = mid and piece == 0
        if is_mid:
            row = half
            for field in range(3):
                arrived[piece, field, pl.ds(half_columns, half_columns), :] = arrived[
                    piece, field, pl.ds(0, half_columns), :
                ]
            near = lambda f: doubled[f]
        else:
            row = my_rows[piece - mid]
            near = lambda f: masked[row, f]
        far = lambda f: arrived[piece, f]
        heat, moment = transform(other, near, far)
        if is_mid:
            given[piece, 0] = jnp.where(left_lanes, heat, moment).astype(BF16)
        else:
            given[piece, 0] = heat.astype(BF16)
            given[piece, 1] = moment.astype(BF16)
        sent = pl.ds(0, rows_sent)
        copies = [
            remote(
                given.at[piece, which, sent, :],
                returned.at[piece, which, sent, :],
                back_send.at[piece, which],
                back_recv.at[piece, which],
            )
            for which in range(1 if is_mid else 2)
        ]
        for copy in copies:
            copy.start()
        back_copies.append(copies)
        heat, moment = transform(me, near, far)
        heat_ref[row] = heat[:rows]
        moment_ref[row] = moment[:rows]

    def mean_to(step):
        peer = (mine + step) % groups
        return pltpu.make_async_remote_copy(
            src_ref=mean_mine,
            dst_ref=gathered.at[mine],
            send_sem=mean_send.at[step],
            recv_sem=mean_recv.at[mine],
            device_id={"lat": peer // lev_ways, "lev": peer % lev_ways},
            device_id_type=pl.DeviceIdType.MESH,
        )

    def mean_from(step):
        peer = (mine + step) % groups
        return pltpu.make_async_remote_copy(
            src_ref=mean_mine,
            dst_ref=gathered.at[peer],
            send_sem=mean_send.at[step],
            recv_sem=mean_recv.at[peer],
            device_id={"lat": peer // lev_ways, "lev": peer % lev_ways},
            device_id_type=pl.DeviceIdType.MESH,
        )

    def share_means():
        zonal_copy.wait_recv()
        total = zonal_mine[...] + zonal_theirs[...]
        mean_mine[...] = jnp.zeros_like(mean_mine)
        mean_mine[pl.ds(0, slab), :] = total[:slab] / jnp.maximum(total[slab:], 1.0)
        target = jnp.concatenate([target_ref[:, b, :] for b in range(batch)], axis=1)
        mean_mine[pl.ds(slab, bands), :] = target
        gathered[mine] = mean_mine[...]

        def start(step, carry):
            mean_to(step).start()
            return carry

        lax.fori_loop(1, groups, start, 0)

    def finish_stream():
        def arrive(step, carry):
            mean_from(step).wait_recv()
            return carry

        lax.fori_loop(1, groups, arrive, 0)
        height = groups * slab
        cosine = cosine_ref[...]
        depth = jnp.concatenate([depth_ref[...]] * batch, axis=1)
        mean = gathered[:, 0:slab, :].reshape(height, columns)
        target = gathered[:, slab : 2 * slab, :].reshape(height, columns)
        stream = mean * cosine * depth
        lane = lax.broadcasted_iota(jnp.int32, (height, columns), 1) % levels
        line = lax.broadcasted_iota(jnp.int32, (height, columns), 0)
        step = 1
        while step < levels:
            stream = stream + jnp.where(lane >= step, pltpu.roll(stream, step, 1), 0.0)
            step *= 2
        step = 1
        while step < height:
            stream = stream + jnp.where(line >= step, pltpu.roll(stream, step, 0), 0.0)
            step *= 2
        peak = jnp.max(jnp.abs(stream))
        stream = stream / (peak + epsilon)
        misfit = jnp.sum(cosine * (stream - target) ** 2)
        penalty_ref[...] = jnp.full((1, 1), misfit / (columns * bands * groups), F32)
        stream_buf[...] = stream
        own = stream_buf[pl.ds(pl.multiple_of(mine * slab, slab), slab), :][:bands]
        for b in range(batch):
            psi_ref[:, b, :] = own[:, b * levels : (b + 1) * levels]

    pieces = mid + half
    for piece in range(pieces):
        if piece == min(1, pieces - 1):
            share_means()
        if piece == pieces - 1:
            finish_stream()
        process(piece)

    for piece in range(pieces):
        for copy in back_copies[piece]:
            copy.wait_recv()
        if mid and piece == 0:
            both = returned[piece, 0].astype(F32)[:rows]
            turned = pltpu.roll(both, half_columns, 1)
            mine_lanes = (lax.broadcasted_iota(jnp.int32, (1, columns), 1) // half_columns) == me
            first = me == 0
            heat_far = jnp.where(first, turned, both)
            moment_far = jnp.where(first, both, turned)
            heat_ref[half] = jnp.where(mine_lanes, heat_ref[half], heat_far)
            moment_ref[half] = jnp.where(mine_lanes, moment_ref[half], moment_far)
        else:
            row = their_rows[piece - mid]
            heat_ref[row] = returned[piece, 0].astype(F32)[:rows]
            moment_ref[row] = returned[piece, 1].astype(F32)[:rows]

    for copies in field_copies + back_copies:
        for copy in copies:
            copy.wait_send()
    zonal_copy.wait_send()

    def sent_all(step, carry):
        mean_to(step).wait_send()
        return carry

    lax.fori_loop(1, groups, sent_all, 0)


def per_device(mesh_shape, u, v, t, keep, depth, target):
    bands, batch, levels, span = v.shape
    lon_ways = mesh_shape["lon"]
    assert lon_ways == 2
    lev_ways = mesh_shape["lev"]
    groups = mesh_shape["lat"] * lev_ways
    rows = HARMONIC_ORDERS // lon_ways
    padded = round_up(rows, 128)
    rows_sent = round_up(rows, 16)
    columns = batch * levels
    half, mid = bands // 2, bands % 2
    pieces = half + mid
    slab = round_up(bands, 8)
    nlat = bands * groups
    table = jnp.asarray(wave_table(span * lon_ways, lon_ways, rows, padded, span))
    latitude = ((np.arange(nlat).astype(np.float32) + np.float32(0.5)) / np.float32(nlat) - np.float32(0.5)) * np.float32(math.pi)
    cosine = np.zeros((groups, slab, 1), np.float32)
    cosine[:, :bands, 0] = np.cos(latitude).reshape(groups, bands)
    cosine = jnp.asarray(np.broadcast_to(cosine.reshape(groups * slab, 1), (groups * slab, columns)).copy())
    fields = [x.reshape(bands, columns, span) for x in (u, v, t)]
    sizes = (bands, batch, levels, span, rows, rows_sent, groups, lev_ways)
    anywhere = pl.BlockSpec(memory_space=pl.ANY)
    inside = pl.BlockSpec(memory_space=pltpu.VMEM)
    psi, heat, moment, penalty = pl.pallas_call(
        functools.partial(kernel, sizes),
        out_shape=(
            jax.ShapeDtypeStruct((bands, batch, levels), F32),
            jax.ShapeDtypeStruct((bands, rows, columns), F32),
            jax.ShapeDtypeStruct((bands, rows, columns), F32),
            jax.ShapeDtypeStruct((1, 1), F32),
        ),
        in_specs=[anywhere] * 5 + [inside] * 3,
        out_specs=(inside,) * 4,
        scratch_shapes=[
            pltpu.VMEM((bands, 3, columns, span), BF16),
            pltpu.VMEM((bands, levels, span), jnp.int32),
            pltpu.VMEM((bands, 3, columns, span), BF16),
            pltpu.VMEM((3, columns, span), BF16),
            pltpu.VMEM((pieces, 3, columns, span), BF16),
            pltpu.VMEM(table.shape, BF16),
            pltpu.VMEM((pieces, 2, padded, columns), BF16),
            pltpu.VMEM((pieces, 2, padded, columns), BF16),
            pltpu.VMEM((2 * slab, columns), F32),
            pltpu.VMEM((2 * slab, columns), F32),
            pltpu.VMEM((2 * slab, columns), F32),
            pltpu.VMEM((groups, 2 * slab, columns), F32),
            pltpu.VMEM((groups * slab, columns), F32),
            pltpu.SemaphoreType.DMA((bands, 4)),
            pltpu.SemaphoreType.DMA,
            pltpu.SemaphoreType.DMA((pieces, 3)),
            pltpu.SemaphoreType.DMA((pieces, 3)),
            pltpu.SemaphoreType.DMA((pieces, 2)),
            pltpu.SemaphoreType.DMA((pieces, 2)),
            pltpu.SemaphoreType.DMA((2,)),
            pltpu.SemaphoreType.DMA((groups,)),
            pltpu.SemaphoreType.DMA((groups,)),
        ],
        compiler_params=pltpu.CompilerParams(
            has_side_effects=True, vmem_limit_bytes=56 * 1024 * 1024
        ),
    )(*fields, keep, table, cosine, depth.reshape(1, levels), target)
    return psi, heat.transpose(1, 0, 2), moment.transpose(1, 0, 2), penalty.reshape(())


def solution(mesh):
    banded = ("lat", "lev")
    placed = (
        P(banded, None, None, "lon"),
        P(banded, None, None, "lon"),
        P(banded, None, None, "lon"),
        P(banded, None, "lon"),
        P(),
        P(banded, None, None),
    )
    return jax.shard_map(
        functools.partial(per_device, dict(mesh.shape)),
        mesh=mesh,
        in_specs=placed,
        out_specs=(P(banded, None, None), P("lon", banded, None), P("lon", banded, None), P()),
        check_vma=False,
    )
```

```python
import functools
import math

import jax
import jax.numpy as jnp
import numpy as np
from jax import lax
from jax.experimental import pallas as pl
from jax.experimental.pallas import tpu as pltpu
from jax.sharding import PartitionSpec as P

HARMONIC_ORDERS = 720
epsilon = 1e-06
F32 = jnp.float32
BF16 = jnp.bfloat16


def round_up(value, step):
    return -(-value // step) * step


def wave_table(meridians, parts, rows, padded, span):
    wavenumber = np.arange(1, HARMONIC_ORDERS + 1, dtype=np.int64)
    turns = (wavenumber[:, None] * np.arange(span)[None, :]) % meridians
    angle = turns.astype(np.float32) * np.float32(2.0 * math.pi / meridians)
    waves = np.stack([np.cos(angle), np.sin(angle)]).astype(np.float32)
    waves = waves.reshape(2, parts, rows, span).transpose(1, 0, 2, 3)
    table = np.zeros((parts, 2, padded, span), np.float32)
    table[:, :, :rows] = waves
    return table.astype(jnp.bfloat16)


def nt_dot(a, b):
    return lax.dot_general(a, b, (((1,), (1,)), ((), ())), preferred_element_type=F32)


def kernel(
    sizes,
    u_ref,
    v_ref,
    t_ref,
    keep_ref,
    table_ref,
    cosine_ref,
    depth_ref,
    target_ref,
    psi_ref,
    own_ref,
    returned,
    penalty_ref,
    raw,
    keep,
    masked,
    doubled,
    packed,
    arrived,
    table,
    given,
    zonal_mine,
    zonal_theirs,
    mean_mine,
    gathered,
    stream_buf,
    load_sem,
    table_sem,
    field_send,
    field_recv,
    back_send,
    back_recv,
    zonal_sem,
    mean_send,
    mean_recv,
):
    bands, batch, levels, span, rows, rows_sent, groups, lev_ways = sizes
    columns = batch * levels
    padded_rows = table.shape[2]
    half, mid = bands // 2, bands % 2
    half_columns = columns // 2
    slab = mean_mine.shape[0] // 2
    me = lax.axis_index("lon")
    other = 1 - me
    mine = lax.axis_index("lat") * lev_ways + lax.axis_index("lev")
    partner = {"lon": other}
    norm_factor = 2.0 / (4.0 * span * span)
    body = span // 128 * 128
    tail = span - body
    whole = lambda step: (mine + step) % groups
    place_of = lambda peer: {"lat": peer // lev_ways, "lev": peer % lev_ways}

    barrier = pltpu.get_barrier_semaphore()
    pl.semaphore_signal(barrier, inc=1, device_id=partner, device_id_type=pl.DeviceIdType.MESH)

    def greet(step, carry):
        pl.semaphore_signal(
            barrier, inc=1, device_id=place_of(whole(step)), device_id_type=pl.DeviceIdType.MESH
        )
        return carry

    lax.fori_loop(1, groups, greet, 0)

    their_rows = [other * (half + mid) + i for i in range(half)]
    my_rows = [me * (half + mid) + i for i in range(half)]
    order = ([half] if mid else []) + their_rows + my_rows

    loads = []
    for place, row in enumerate(order):
        loads.append(
            [
                pltpu.make_async_copy(keep_ref.at[row], keep.at[row], load_sem.at[place, 3]),
                pltpu.make_async_copy(u_ref.at[row], raw.at[row, 0], load_sem.at[place, 0]),
                pltpu.make_async_copy(v_ref.at[row], raw.at[row, 1], load_sem.at[place, 1]),
                pltpu.make_async_copy(t_ref.at[row], raw.at[row, 2], load_sem.at[place, 2]),
            ]
        )
        for copy in loads[-1]:
            copy.start()
    table_load = pltpu.make_async_copy(table_ref, table, table_sem)
    table_load.start()

    def mask_row(place):
        row = order[place]
        for copy in loads[place]:
            copy.wait()
        ones = keep[row].astype(F32).astype(BF16)
        for field in range(3):
            for sample in range(batch):
                part = pl.ds(sample * levels, levels)
                masked[row, field, part, :] = raw[row, field, part, :] * ones

    def remote(src, dst, send, recv):
        return pltpu.make_async_remote_copy(
            src_ref=src,
            dst_ref=dst,
            send_sem=send,
            recv_sem=recv,
            device_id=partner,
            device_id_type=pl.DeviceIdType.MESH,
        )

    field_copies = []

    def pack_row(piece, place):
        row = order[place]
        if mid and piece == 0:
            away = pl.ds(pl.multiple_of(other * half_columns, half_columns), half_columns)
            here = pl.ds(0, half_columns)
        else:
            away = here = pl.ds(0, columns)
        ends = []
        for field in range(3):
            packed[piece, here, pl.ds(field * body, body)] = masked[row, field, away, pl.ds(0, body)]
            ends.append(masked[row, field, away, pl.ds(body, tail)])
        packed[piece, here, pl.ds(3 * body, 3 * tail)] = jnp.concatenate(ends, axis=1)
        return here

    def send_row(piece, place):
        here = pack_row(piece, place)
        if place == 0:
            pl.semaphore_wait(barrier, groups)
        copy = remote(
            packed.at[piece, here, :],
            arrived.at[piece, here, :],
            field_send.at[piece],
            field_recv.at[piece],
        )
        copy.start()
        field_copies.append([copy])

    def far_field(piece, field):
        bulk = arrived[piece, :, pl.ds(field * body, body)]
        end = arrived[piece, :, pl.ds(3 * body + field * tail, tail)]
        return jnp.concatenate([bulk, end], axis=1)

    early = min(mid + 1, mid + half)
    for place in range(early):
        mask_row(place)
        send_row(place, place)
    for place in range(early, len(order)):
        mask_row(place)

    ones_row = jnp.ones((8, span), BF16)
    zonal_mine[...] = jnp.zeros_like(zonal_mine)
    for row in range(bands):
        zonal_mine[pl.ds(row, 1), :] = nt_dot(ones_row, masked[row, 1])[0:1]
        counts = nt_dot(ones_row, keep[row].astype(F32).astype(BF16))[0:1]
        zonal_mine[pl.ds(slab + row, 1), :] = jnp.concatenate([counts] * batch, axis=1)
    zonal_copy = remote(zonal_mine, zonal_theirs, zonal_sem.at[0], zonal_sem.at[1])
    zonal_copy.start()
    for place in range(early, mid + half):
        send_row(place, place)

    if mid:
        here = pl.ds(pl.multiple_of(me * half_columns, half_columns), half_columns)
        for field in range(3):
            own = masked[half, field, here, :]
            doubled[field, pl.ds(0, half_columns), :] = own
            doubled[field, pl.ds(half_columns, half_columns), :] = own
    table_load.wait()

    row_index = lax.broadcasted_iota(jnp.int32, (padded_rows, 1), 0)
    left_lanes = lax.broadcasted_iota(jnp.int32, (1, columns), 1) < half_columns
    back_copies = []

    def transform(part, near, far):
        parity = (row_index + 1 + part * rows) % 2
        sign = (1 - 2 * parity).astype(F32)
        pieces = []
        for trig in range(2):
            wave = table[part, trig]
            pieces.append([nt_dot(wave, near(f)) + sign * nt_dot(wave, far(f)) for f in range(3)])
        (uc, vc, tc), (us, vs, ts) = pieces
        return norm_factor * (vc * tc + vs * ts), norm_factor * (uc * vc + us * vs)

    def process(piece):
        for copy in field_copies[piece]:
            copy.wait_recv()
        is_mid = mid and piece == 0
        if is_mid:
            arrived[piece, pl.ds(half_columns, half_columns), :] = arrived[
                piece, pl.ds(0, half_columns), :
            ]
            near = lambda f: doubled[f]
        else:
            row = my_rows[piece - mid]
            near = lambda f: masked[row, f]
        far = lambda f: far_field(piece, f)
        heat, moment = transform(other, near, far)
        if is_mid:
            given[piece, 0] = jnp.where(left_lanes, heat, moment).astype(BF16)
        else:
            given[piece, 0] = heat.astype(BF16)
            given[piece, 1] = moment.astype(BF16)
        sent = pl.ds(0, rows_sent)
        copies = [
            remote(
                given.at[piece, which, sent, :],
                returned.at[piece, which, sent, :],
                back_send.at[piece, which],
                back_recv.at[piece, which],
            )
            for which in range(1 if is_mid else 2)
        ]
        for copy in copies:
            copy.start()
        back_copies.append(copies)
        heat, moment = transform(me, near, far)
        own_ref[piece, 0] = heat[:rows]
        own_ref[piece, 1] = moment[:rows]

    def mean_to(step):
        peer = whole(step)
        return pltpu.make_async_remote_copy(
            src_ref=mean_mine,
            dst_ref=gathered.at[mine],
            send_sem=mean_send.at[step],
            recv_sem=mean_recv.at[mine],
            device_id=place_of(peer),
            device_id_type=pl.DeviceIdType.MESH,
        )

    def mean_from(step):
        peer = whole(step)
        return pltpu.make_async_remote_copy(
            src_ref=mean_mine,
            dst_ref=gathered.at[peer],
            send_sem=mean_send.at[step],
            recv_sem=mean_recv.at[peer],
            device_id=place_of(peer),
            device_id_type=pl.DeviceIdType.MESH,
        )

    def share_means():
        zonal_copy.wait_recv()
        total = zonal_mine[...] + zonal_theirs[...]
        mean_mine[...] = jnp.zeros_like(mean_mine)
        mean_mine[pl.ds(0, slab), :] = total[:slab] / jnp.maximum(total[slab:], 1.0)
        target = jnp.concatenate([target_ref[:, b, :] for b in range(batch)], axis=1)
        mean_mine[pl.ds(slab, bands), :] = target
        gathered[mine] = mean_mine[...]

        def start(step, carry):
            mean_to(step).start()
            return carry

        lax.fori_loop(1, groups, start, 0)

    def finish_stream():
        def arrive(step, carry):
            mean_from(step).wait_recv()
            return carry

        lax.fori_loop(1, groups, arrive, 0)
        height = groups * slab
        cosine = cosine_ref[...]
        depth = jnp.concatenate([depth_ref[...]] * batch, axis=1)
        mean = gathered[:, 0:slab, :].reshape(height, columns)
        target = gathered[:, slab : 2 * slab, :].reshape(height, columns)
        stream = mean * cosine * depth
        lane = lax.broadcasted_iota(jnp.int32, (height, columns), 1) % levels
        line = lax.broadcasted_iota(jnp.int32, (height, columns), 0)
        step = 1
        while step < levels:
            stream = stream + jnp.where(lane >= step, pltpu.roll(stream, step, 1), 0.0)
            step *= 2
        step = 1
        while step < height:
            stream = stream + jnp.where(line >= step, pltpu.roll(stream, step, 0), 0.0)
            step *= 2
        peak = jnp.max(jnp.abs(stream))
        stream = stream / (peak + epsilon)
        misfit = jnp.sum(cosine * (stream - target) ** 2)
        penalty_ref[...] = jnp.full((1, 1), misfit / (columns * bands * groups), F32)
        stream_buf[...] = stream
        own = stream_buf[pl.ds(pl.multiple_of(mine * slab, slab), slab), :][:bands]
        for b in range(batch):
            psi_ref[:, b, :] = own[:, b * levels : (b + 1) * levels]

    pieces = mid + half
    for piece in range(pieces):
        if piece == min(1, pieces - 1):
            share_means()
        if piece == pieces - 1:
            finish_stream()
        process(piece)

    for copies in back_copies:
        for copy in copies:
            copy.wait_recv()
    for copies in field_copies + back_copies:
        for copy in copies:
            copy.wait_send()
    zonal_copy.wait_send()

    def sent_all(step, carry):
        mean_to(step).wait_send()
        return carry

    lax.fori_loop(1, groups, sent_all, 0)


def assemble(sizes, psi_in, own_ref, returned, penalty_in, psi_ref, heat_ref, moment_ref, penalty_ref, stage, sems):
    bands, batch, levels, rows = sizes
    columns = batch * levels
    half, mid = bands // 2, bands % 2
    half_columns = columns // 2
    me = lax.axis_index("lon")
    other = 1 - me
    copies = []

    def put(row, slot, heat, moment):
        stage[slot, 0] = heat
        stage[slot, 1] = moment
        for which, out in enumerate((heat_ref, moment_ref)):
            copy = pltpu.make_async_copy(stage.at[slot, which], out.at[row], sems.at[slot, which])
            copy.start()
            copies.append(copy)

    for i in range(half):
        piece = mid + i
        for which, out in enumerate((heat_ref, moment_ref)):
            copy = pltpu.make_async_copy(
                own_ref.at[piece, which], out.at[me * (half + mid) + i], sems.at[half + mid + i, which]
            )
            copy.start()
            copies.append(copy)
    for i in range(half):
        piece = mid + i
        put(
            other * (half + mid) + i,
            piece,
            returned[piece, 0, :rows].astype(F32),
            returned[piece, 1, :rows].astype(F32),
        )
    if mid:
        both = returned[0, 0, :rows].astype(F32)
        turned = pltpu.roll(both, half_columns, 1)
        mine_lanes = (lax.broadcasted_iota(jnp.int32, (1, columns), 1) // half_columns) == me
        first = me == 0
        put(
            half,
            0,
            jnp.where(mine_lanes, own_ref[0, 0], jnp.where(first, turned, both)),
            jnp.where(mine_lanes, own_ref[0, 1], jnp.where(first, both, turned)),
        )
    psi_ref[...] = psi_in[...]
    penalty_ref[...] = penalty_in[...]
    for copy in copies:
        copy.wait()


def per_device(mesh_shape, u, v, t, keep, depth, target):
    bands, batch, levels, span = v.shape
    lon_ways = mesh_shape["lon"]
    assert lon_ways == 2
    lev_ways = mesh_shape["lev"]
    groups = mesh_shape["lat"] * lev_ways
    rows = HARMONIC_ORDERS // lon_ways
    padded = round_up(rows, 128)
    rows_sent = round_up(rows, 16)
    columns = batch * levels
    half, mid = bands // 2, bands % 2
    pieces = half + mid
    slab = round_up(bands, 8)
    nlat = bands * groups
    table = jnp.asarray(wave_table(span * lon_ways, lon_ways, rows, padded, span))
    latitude = ((np.arange(nlat).astype(np.float32) + np.float32(0.5)) / np.float32(nlat) - np.float32(0.5)) * np.float32(math.pi)
    cosine = np.zeros((groups, slab, 1), np.float32)
    cosine[:, :bands, 0] = np.cos(latitude).reshape(groups, bands)
    cosine = jnp.asarray(np.broadcast_to(cosine.reshape(groups * slab, 1), (groups * slab, columns)).copy())
    fields = [x.reshape(bands, columns, span) for x in (u, v, t)]
    sizes = (bands, batch, levels, span, rows, rows_sent, groups, lev_ways)
    anywhere = pl.BlockSpec(memory_space=pl.ANY)
    inside = pl.BlockSpec(memory_space=pltpu.VMEM)
    in_hbm = pl.BlockSpec(memory_space=pltpu.MemorySpace.HBM)
    body = span // 128 * 128
    lanes = 3 * body + round_up(3 * (span - body), 128)
    mid_results = pl.pallas_call(
        functools.partial(kernel, sizes),
        out_shape=(
            jax.ShapeDtypeStruct((bands, batch, levels), F32),
            jax.ShapeDtypeStruct((pieces, 2, rows, columns), F32),
            jax.ShapeDtypeStruct((pieces, 2, padded, columns), BF16),
            jax.ShapeDtypeStruct((1, 1), F32),
        ),
        in_specs=[in_hbm] * 5 + [inside] * 3,
        out_specs=(inside,) * 4,
        scratch_shapes=[
            pltpu.VMEM((bands, 3, columns, span), BF16),
            pltpu.VMEM((bands, levels, span), jnp.int32),
            pltpu.VMEM((bands, 3, columns, span), BF16),
            pltpu.VMEM((3, columns, span), BF16),
            pltpu.VMEM((pieces, columns, lanes), BF16),
            pltpu.VMEM((pieces, columns, lanes), BF16),
            pltpu.VMEM(table.shape, BF16),
            pltpu.VMEM((pieces, 2, padded, columns), BF16),
            pltpu.VMEM((2 * slab, columns), F32),
            pltpu.VMEM((2 * slab, columns), F32),
            pltpu.VMEM((2 * slab, columns), F32),
            pltpu.VMEM((groups, 2 * slab, columns), F32),
            pltpu.VMEM((groups * slab, columns), F32),
            pltpu.SemaphoreType.DMA((bands, 4)),
            pltpu.SemaphoreType.DMA,
            pltpu.SemaphoreType.DMA((pieces,)),
            pltpu.SemaphoreType.DMA((pieces,)),
            pltpu.SemaphoreType.DMA((pieces, 2)),
            pltpu.SemaphoreType.DMA((pieces, 2)),
            pltpu.SemaphoreType.DMA((2,)),
            pltpu.SemaphoreType.DMA((groups,)),
            pltpu.SemaphoreType.DMA((groups,)),
        ],
        compiler_params=pltpu.CompilerParams(
            collective_id=0, has_side_effects=True, vmem_limit_bytes=32 * 1024 * 1024
        ),
    )(*fields, keep, table, cosine, depth.reshape(1, levels), target)
    psi, heat, moment, penalty = pl.pallas_call(
        functools.partial(assemble, (bands, batch, levels, rows)),
        out_shape=(
            jax.ShapeDtypeStruct((bands, batch, levels), F32),
            jax.ShapeDtypeStruct((bands, rows, columns), F32),
            jax.ShapeDtypeStruct((bands, rows, columns), F32),
            jax.ShapeDtypeStruct((1, 1), F32),
        ),
        in_specs=[inside] * 4,
        out_specs=(inside, anywhere, anywhere, inside),
        scratch_shapes=[
            pltpu.VMEM((pieces, 2, rows, columns), F32),
            pltpu.SemaphoreType.DMA((pieces + half, 2)),
        ],
        compiler_params=pltpu.CompilerParams(vmem_limit_bytes=8 * 1024 * 1024),
    )(*mid_results)
    return psi, heat.transpose(1, 0, 2), moment.transpose(1, 0, 2), penalty.reshape(())


def solution(mesh):
    banded = ("lat", "lev")
    placed = (
        P(banded, None, None, "lon"),
        P(banded, None, None, "lon"),
        P(banded, None, None, "lon"),
        P(banded, None, "lon"),
        P(),
        P(banded, None, None),
    )
    return jax.shard_map(
        functools.partial(per_device, dict(mesh.shape)),
        mesh=mesh,
        in_specs=placed,
        out_specs=(P(banded, None, None), P("lon", banded, None), P("lon", banded, None), P()),
        check_vma=False,
    )
```

```python
import functools
import math

import jax
import jax.numpy as jnp
import numpy as np
from jax import lax
from jax.experimental import pallas as pl
from jax.experimental.pallas import tpu as pltpu
from jax.sharding import PartitionSpec as P

HARMONIC_ORDERS = 720
epsilon = 1e-06
F32 = jnp.float32
BF16 = jnp.bfloat16


def round_up(value, step):
    return -(-value // step) * step


def wave_table(meridians, parts, rows, padded, span):
    wavenumber = np.arange(1, HARMONIC_ORDERS + 1, dtype=np.int64)
    turns = (wavenumber[:, None] * np.arange(span)[None, :]) % meridians
    angle = turns.astype(np.float32) * np.float32(2.0 * math.pi / meridians)
    waves = np.stack([np.cos(angle), np.sin(angle)]).astype(np.float32)
    waves = waves.reshape(2, parts, rows, span).transpose(1, 0, 2, 3)
    table = np.zeros((parts, 2, padded, span), np.float32)
    table[:, :, :rows] = waves
    return table.astype(jnp.bfloat16)


def nt_dot(a, b):
    return lax.dot_general(a, b, (((1,), (1,)), ((), ())), preferred_element_type=F32)


def kernel(
    sizes,
    u_ref,
    v_ref,
    t_ref,
    keep_ref,
    table_ref,
    cosine_ref,
    depth_ref,
    target_ref,
    psi_ref,
    own_ref,
    returned,
    penalty_ref,
    raw,
    keep,
    masked,
    doubled,
    packed,
    arrived,
    table,
    given,
    zonal_mine,
    zonal_theirs,
    mean_mine,
    gathered,
    stream_buf,
    load_sem,
    table_sem,
    field_send,
    field_recv,
    back_send,
    back_recv,
    zonal_sem,
    mean_send,
    mean_recv,
):
    bands, batch, levels, span, rows, rows_sent, groups, lev_ways = sizes
    columns = batch * levels
    padded_rows = table.shape[2]
    half, mid = bands // 2, bands % 2
    half_columns = columns // 2
    slab = mean_mine.shape[0] // 2
    me = lax.axis_index("lon")
    other = 1 - me
    mine = lax.axis_index("lat") * lev_ways + lax.axis_index("lev")
    partner = {"lon": other}
    norm_factor = 2.0 / (4.0 * span * span)
    body = span // 128 * 128
    tail = span - body
    whole = lambda step: (mine + step) % groups
    place_of = lambda peer: {"lat": peer // lev_ways, "lev": peer % lev_ways}

    barrier = pltpu.get_barrier_semaphore()
    pl.semaphore_signal(barrier, inc=1, device_id=partner, device_id_type=pl.DeviceIdType.MESH)

    def greet(step, carry):
        pl.semaphore_signal(
            barrier, inc=1, device_id=place_of(whole(step)), device_id_type=pl.DeviceIdType.MESH
        )
        return carry

    lax.fori_loop(1, groups, greet, 0)

    their_rows = [other * (half + mid) + i for i in range(half)]
    my_rows = [me * (half + mid) + i for i in range(half)]
    order = ([half] if mid else []) + their_rows + my_rows

    loads = []
    for place, row in enumerate(order):
        loads.append(
            [
                pltpu.make_async_copy(keep_ref.at[row], keep.at[row], load_sem.at[place, 3]),
                pltpu.make_async_copy(u_ref.at[row], raw.at[row, 0], load_sem.at[place, 0]),
                pltpu.make_async_copy(v_ref.at[row], raw.at[row, 1], load_sem.at[place, 1]),
                pltpu.make_async_copy(t_ref.at[row], raw.at[row, 2], load_sem.at[place, 2]),
            ]
        )
        for copy in loads[-1]:
            copy.start()
    table_load = pltpu.make_async_copy(table_ref, table, table_sem)
    table_load.start()

    def mask_row(place):
        row = order[place]
        for copy in loads[place]:
            copy.wait()
        ones = keep[row].astype(F32).astype(BF16)
        for field in range(3):
            for sample in range(batch):
                part = pl.ds(sample * levels, levels)
                masked[row, field, part, :] = raw[row, field, part, :] * ones

    def remote(src, dst, send, recv):
        return pltpu.make_async_remote_copy(
            src_ref=src,
            dst_ref=dst,
            send_sem=send,
            recv_sem=recv,
            device_id=partner,
            device_id_type=pl.DeviceIdType.MESH,
        )

    field_copies = []

    def pack_row(piece, place):
        row = order[place]
        if mid and piece == 0:
            away = pl.ds(pl.multiple_of(other * half_columns, half_columns), half_columns)
            here = pl.ds(0, half_columns)
        else:
            away = here = pl.ds(0, columns)
        ends = []
        for field in range(3):
            packed[piece, here, pl.ds(field * body, body)] = masked[row, field, away, pl.ds(0, body)]
            ends.append(masked[row, field, away, pl.ds(body, tail)])
        packed[piece, here, pl.ds(3 * body, 3 * tail)] = jnp.concatenate(ends, axis=1)
        return here

    def send_row(piece, place):
        here = pack_row(piece, place)
        if place == 0:
            pl.semaphore_wait(barrier, groups)
        copy = remote(
            packed.at[piece, here, :],
            arrived.at[piece, here, :],
            field_send.at[piece],
            field_recv.at[piece],
        )
        copy.start()
        field_copies.append([copy])

    def far_field(piece, field):
        bulk = arrived[piece, :, pl.ds(field * body, body)]
        end = arrived[piece, :, pl.ds(3 * body + field * tail, tail)]
        return jnp.concatenate([bulk, end], axis=1)

    early = min(mid + 1, mid + half)
    for place in range(early):
        mask_row(place)
        send_row(place, place)
    for place in range(early, len(order)):
        mask_row(place)

    ones_row = jnp.ones((8, span), BF16)
    zonal_mine[...] = jnp.zeros_like(zonal_mine)
    for row in range(bands):
        zonal_mine[pl.ds(row, 1), :] = nt_dot(ones_row, masked[row, 1])[0:1]
        counts = nt_dot(ones_row, keep[row].astype(F32).astype(BF16))[0:1]
        zonal_mine[pl.ds(slab + row, 1), :] = jnp.concatenate([counts] * batch, axis=1)
    zonal_copy = remote(zonal_mine, zonal_theirs, zonal_sem.at[0], zonal_sem.at[1])
    zonal_copy.start()
    for place in range(early, mid + half):
        send_row(place, place)

    if mid:
        here = pl.ds(pl.multiple_of(me * half_columns, half_columns), half_columns)
        for field in range(3):
            own = masked[half, field, here, :]
            doubled[field, pl.ds(0, half_columns), :] = own
            doubled[field, pl.ds(half_columns, half_columns), :] = own
    table_load.wait()

    row_index = lax.broadcasted_iota(jnp.int32, (padded_rows, 1), 0)
    left_lanes = lax.broadcasted_iota(jnp.int32, (1, columns), 1) < half_columns
    back_copies = []

    def transform(part, near, far):
        parity = (row_index + 1 + part * rows) % 2
        sign = (1 - 2 * parity).astype(F32)
        pieces = []
        for trig in range(2):
            wave = table[part, trig]
            pieces.append([nt_dot(wave, near(f)) + sign * nt_dot(wave, far(f)) for f in range(3)])
        (uc, vc, tc), (us, vs, ts) = pieces
        return norm_factor * (vc * tc + vs * ts), norm_factor * (uc * vc + us * vs)

    def process(piece):
        for copy in field_copies[piece]:
            copy.wait_recv()
        is_mid = mid and piece == 0
        if is_mid:
            arrived[piece, pl.ds(half_columns, half_columns), :] = arrived[
                piece, pl.ds(0, half_columns), :
            ]
            near = lambda f: doubled[f]
        else:
            row = my_rows[piece - mid]
            near = lambda f: masked[row, f]
        far = lambda f: far_field(piece, f)
        heat, moment = transform(other, near, far)
        if is_mid:
            given[piece, 0] = jnp.where(left_lanes, heat, moment).astype(BF16)
        else:
            given[piece, 0] = heat.astype(BF16)
            given[piece, 1] = moment.astype(BF16)
        sent = pl.ds(0, rows_sent)
        copies = [
            remote(
                given.at[piece, which, sent, :],
                returned.at[piece, which, sent, :],
                back_send.at[piece, which],
                back_recv.at[piece, which],
            )
            for which in range(1 if is_mid else 2)
        ]
        for copy in copies:
            copy.start()
        back_copies.append(copies)
        heat, moment = transform(me, near, far)
        own_ref[piece, 0] = heat[:rows]
        own_ref[piece, 1] = moment[:rows]

    def mean_to(step):
        peer = whole(step)
        return pltpu.make_async_remote_copy(
            src_ref=mean_mine,
            dst_ref=gathered.at[mine],
            send_sem=mean_send.at[step],
            recv_sem=mean_recv.at[mine],
            device_id=place_of(peer),
            device_id_type=pl.DeviceIdType.MESH,
        )

    def mean_from(step):
        peer = whole(step)
        return pltpu.make_async_remote_copy(
            src_ref=mean_mine,
            dst_ref=gathered.at[peer],
            send_sem=mean_send.at[step],
            recv_sem=mean_recv.at[peer],
            device_id=place_of(peer),
            device_id_type=pl.DeviceIdType.MESH,
        )

    def share_means():
        zonal_copy.wait_recv()
        total = zonal_mine[...] + zonal_theirs[...]
        mean_mine[...] = jnp.zeros_like(mean_mine)
        mean_mine[pl.ds(0, slab), :] = total[:slab] / jnp.maximum(total[slab:], 1.0)
        target = jnp.concatenate([target_ref[:, b, :] for b in range(batch)], axis=1)
        mean_mine[pl.ds(slab, bands), :] = target
        gathered[mine] = mean_mine[...]

        def start(step, carry):
            mean_to(step).start()
            return carry

        lax.fori_loop(1, groups, start, 0)

    def finish_stream():
        def arrive(step, carry):
            mean_from(step).wait_recv()
            return carry

        lax.fori_loop(1, groups, arrive, 0)
        height = groups * slab
        cosine = cosine_ref[...]
        depth = jnp.concatenate([depth_ref[...]] * batch, axis=1)
        mean = gathered[:, 0:slab, :].reshape(height, columns)
        target = gathered[:, slab : 2 * slab, :].reshape(height, columns)
        stream = mean * cosine * depth
        lane = lax.broadcasted_iota(jnp.int32, (height, columns), 1) % levels
        line = lax.broadcasted_iota(jnp.int32, (height, columns), 0)
        step = 1
        while step < levels:
            stream = stream + jnp.where(lane >= step, pltpu.roll(stream, step, 1), 0.0)
            step *= 2
        step = 1
        while step < height:
            stream = stream + jnp.where(line >= step, pltpu.roll(stream, step, 0), 0.0)
            step *= 2
        peak = jnp.max(jnp.abs(stream))
        stream = stream / (peak + epsilon)
        misfit = jnp.sum(cosine * (stream - target) ** 2)
        penalty_ref[...] = jnp.full((1, 1), misfit / (columns * bands * groups), F32)
        stream_buf[...] = stream
        own = stream_buf[pl.ds(pl.multiple_of(mine * slab, slab), slab), :][:bands]
        for b in range(batch):
            psi_ref[:, b, :] = own[:, b * levels : (b + 1) * levels]

    pieces = mid + half
    for piece in range(pieces):
        if piece == min(1, pieces - 1):
            share_means()
        if piece == pieces - 1:
            finish_stream()
        process(piece)

    for copies in back_copies:
        for copy in copies:
            copy.wait_recv()
    for copies in field_copies + back_copies:
        for copy in copies:
            copy.wait_send()
    zonal_copy.wait_send()

    def sent_all(step, carry):
        mean_to(step).wait_send()
        return carry

    lax.fori_loop(1, groups, sent_all, 0)


def assemble(sizes, psi_in, own_ref, returned, penalty_in, psi_ref, heat_ref, moment_ref, penalty_ref, stage, sems):
    bands, batch, levels, rows = sizes
    columns = batch * levels
    half, mid = bands // 2, bands % 2
    half_columns = columns // 2
    me = lax.axis_index("lon")
    other = 1 - me
    copies = []

    def put(row, slot, heat, moment):
        stage[slot, 0] = heat
        stage[slot, 1] = moment
        for which, out in enumerate((heat_ref, moment_ref)):
            copy = pltpu.make_async_copy(stage.at[slot, which], out.at[row], sems.at[slot, which])
            copy.start()
            copies.append(copy)

    for i in range(half):
        piece = mid + i
        for which, out in enumerate((heat_ref, moment_ref)):
            copy = pltpu.make_async_copy(
                own_ref.at[piece, which], out.at[me * (half + mid) + i], sems.at[half + mid + i, which]
            )
            copy.start()
            copies.append(copy)
    for i in range(half):
        piece = mid + i
        put(
            other * (half + mid) + i,
            piece,
            returned[piece, 0, :rows].astype(F32),
            returned[piece, 1, :rows].astype(F32),
        )
    if mid:
        both = returned[0, 0, :rows].astype(F32)
        turned = pltpu.roll(both, half_columns, 1)
        mine_lanes = (lax.broadcasted_iota(jnp.int32, (1, columns), 1) // half_columns) == me
        first = me == 0
        put(
            half,
            0,
            jnp.where(mine_lanes, own_ref[0, 0], jnp.where(first, turned, both)),
            jnp.where(mine_lanes, own_ref[0, 1], jnp.where(first, both, turned)),
        )
    psi_ref[...] = psi_in[...]
    penalty_ref[...] = penalty_in[...]
    for copy in copies:
        copy.wait()


def per_device(mesh_shape, u, v, t, keep, depth, target):
    bands, batch, levels, span = v.shape
    lon_ways = mesh_shape["lon"]
    assert lon_ways == 2
    lev_ways = mesh_shape["lev"]
    groups = mesh_shape["lat"] * lev_ways
    rows = HARMONIC_ORDERS // lon_ways
    padded = round_up(rows, 128)
    rows_sent = round_up(rows, 16)
    columns = batch * levels
    half, mid = bands // 2, bands % 2
    pieces = half + mid
    slab = round_up(bands, 8)
    nlat = bands * groups
    table = jnp.asarray(wave_table(span * lon_ways, lon_ways, rows, padded, span))
    latitude = ((np.arange(nlat).astype(np.float32) + np.float32(0.5)) / np.float32(nlat) - np.float32(0.5)) * np.float32(math.pi)
    cosine = np.zeros((groups, slab, 1), np.float32)
    cosine[:, :bands, 0] = np.cos(latitude).reshape(groups, bands)
    cosine = jnp.asarray(np.broadcast_to(cosine.reshape(groups * slab, 1), (groups * slab, columns)).copy())
    fields = [x.reshape(bands, columns, span) for x in (u, v, t)]
    sizes = (bands, batch, levels, span, rows, rows_sent, groups, lev_ways)
    anywhere = pl.BlockSpec(memory_space=pl.ANY)
    inside = pl.BlockSpec(memory_space=pltpu.VMEM)
    in_hbm = pl.BlockSpec(memory_space=pltpu.MemorySpace.HBM)
    body = span // 128 * 128
    lanes = 3 * body + round_up(3 * (span - body), 128)
    mid_results = pl.pallas_call(
        functools.partial(kernel, sizes),
        out_shape=(
            pltpu.MemorySpace.VMEM((bands, batch, levels), F32),
            pltpu.MemorySpace.VMEM((pieces, 2, rows, columns), F32),
            pltpu.MemorySpace.VMEM((pieces, 2, padded, columns), BF16),
            pltpu.MemorySpace.VMEM((1, 1), F32),
        ),
        in_specs=[in_hbm] * 5 + [inside] * 3,
        out_specs=(inside,) * 4,
        scratch_shapes=[
            pltpu.VMEM((bands, 3, columns, span), BF16),
            pltpu.VMEM((bands, levels, span), jnp.int32),
            pltpu.VMEM((bands, 3, columns, span), BF16),
            pltpu.VMEM((3, columns, span), BF16),
            pltpu.VMEM((pieces, columns, lanes), BF16),
            pltpu.VMEM((pieces, columns, lanes), BF16),
            pltpu.VMEM(table.shape, BF16),
            pltpu.VMEM((pieces, 2, padded, columns), BF16),
            pltpu.VMEM((2 * slab, columns), F32),
            pltpu.VMEM((2 * slab, columns), F32),
            pltpu.VMEM((2 * slab, columns), F32),
            pltpu.VMEM((groups, 2 * slab, columns), F32),
            pltpu.VMEM((groups * slab, columns), F32),
            pltpu.SemaphoreType.DMA((bands, 4)),
            pltpu.SemaphoreType.DMA,
            pltpu.SemaphoreType.DMA((pieces,)),
            pltpu.SemaphoreType.DMA((pieces,)),
            pltpu.SemaphoreType.DMA((pieces, 2)),
            pltpu.SemaphoreType.DMA((pieces, 2)),
            pltpu.SemaphoreType.DMA((2,)),
            pltpu.SemaphoreType.DMA((groups,)),
            pltpu.SemaphoreType.DMA((groups,)),
        ],
        compiler_params=pltpu.CompilerParams(
            collective_id=0, has_side_effects=True, vmem_limit_bytes=56 * 1024 * 1024
        ),
    )(*fields, keep, table, cosine, depth.reshape(1, levels), target)
    psi, heat, moment, penalty = pl.pallas_call(
        functools.partial(assemble, (bands, batch, levels, rows)),
        out_shape=(
            jax.ShapeDtypeStruct((bands, batch, levels), F32),
            jax.ShapeDtypeStruct((bands, rows, columns), F32),
            jax.ShapeDtypeStruct((bands, rows, columns), F32),
            jax.ShapeDtypeStruct((1, 1), F32),
        ),
        in_specs=[inside] * 4,
        out_specs=(inside, anywhere, anywhere, inside),
        scratch_shapes=[
            pltpu.VMEM((pieces, 2, rows, columns), F32),
            pltpu.SemaphoreType.DMA((pieces + half, 2)),
        ],
        compiler_params=pltpu.CompilerParams(vmem_limit_bytes=8 * 1024 * 1024),
    )(*mid_results)
    return psi, heat.transpose(1, 0, 2), moment.transpose(1, 0, 2), penalty.reshape(())


def solution(mesh):
    banded = ("lat", "lev")
    placed = (
        P(banded, None, None, "lon"),
        P(banded, None, None, "lon"),
        P(banded, None, None, "lon"),
        P(banded, None, "lon"),
        P(),
        P(banded, None, None),
    )
    return jax.shard_map(
        functools.partial(per_device, dict(mesh.shape)),
        mesh=mesh,
        in_specs=placed,
        out_specs=(P(banded, None, None), P("lon", banded, None), P("lon", banded, None), P()),
        check_vma=False,
    )
```

```python
import functools
import math

import jax
import jax.numpy as jnp
import numpy as np
from jax import lax
from jax.experimental import pallas as pl
from jax.experimental.pallas import tpu as pltpu
from jax.sharding import PartitionSpec as P

HARMONIC_ORDERS = 720
epsilon = 1e-06
F32 = jnp.float32
BF16 = jnp.bfloat16


def round_up(value, step):
    return -(-value // step) * step


def wave_table(meridians, parts, rows, padded, span):
    wavenumber = np.arange(1, HARMONIC_ORDERS + 1, dtype=np.int64)
    turns = (wavenumber[:, None] * np.arange(span)[None, :]) % meridians
    angle = turns.astype(np.float32) * np.float32(2.0 * math.pi / meridians)
    waves = np.stack([np.cos(angle), np.sin(angle)]).astype(np.float32)
    waves = waves.reshape(2, parts, rows, span).transpose(1, 0, 2, 3)
    table = np.zeros((parts, 2, padded, span), np.float32)
    table[:, :, :rows] = waves
    return table.astype(jnp.bfloat16)


def nt_dot(a, b):
    return lax.dot_general(a, b, (((1,), (1,)), ((), ())), preferred_element_type=F32)


def kernel(
    sizes,
    u_ref,
    v_ref,
    t_ref,
    keep_ref,
    table_ref,
    cosine_ref,
    depth_ref,
    target_ref,
    psi_ref,
    own_ref,
    returned,
    penalty_ref,
    raw,
    keep,
    masked,
    doubled,
    packed,
    arrived,
    table,
    given,
    zonal_mine,
    zonal_theirs,
    mean_mine,
    gathered,
    stream_buf,
    load_sem,
    table_sem,
    field_send,
    field_recv,
    back_send,
    back_recv,
    zonal_sem,
    mean_send,
    mean_recv,
):
    bands, batch, levels, span, rows, rows_sent, groups, lev_ways = sizes
    columns = batch * levels
    padded_rows = table.shape[2]
    half, mid = bands // 2, bands % 2
    half_columns = columns // 2
    slab = mean_mine.shape[0] // 2
    me = lax.axis_index("lon")
    other = 1 - me
    mine = lax.axis_index("lat") * lev_ways + lax.axis_index("lev")
    partner = {"lon": other}
    norm_factor = 2.0 / (4.0 * span * span)
    body = span // 128 * 128
    tail = span - body
    strides = [2**bit for bit in range(groups.bit_length() - 1)]
    across = lambda stride: mine + stride * (1 - 2 * ((mine // stride) % 2))
    place_of = lambda peer: {"lat": peer // lev_ways, "lev": peer % lev_ways}

    barrier = pltpu.get_barrier_semaphore()
    pl.semaphore_signal(barrier, inc=1, device_id=partner, device_id_type=pl.DeviceIdType.MESH)

    for stride in strides:
        pl.semaphore_signal(
            barrier,
            inc=1,
            device_id=place_of(across(stride)),
            device_id_type=pl.DeviceIdType.MESH,
        )

    their_rows = [other * (half + mid) + i for i in range(half)]
    my_rows = [me * (half + mid) + i for i in range(half)]
    order = ([half] if mid else []) + their_rows + my_rows

    loads = []
    for place, row in enumerate(order):
        loads.append(
            [
                pltpu.make_async_copy(keep_ref.at[row], keep.at[row], load_sem.at[place, 3]),
                pltpu.make_async_copy(u_ref.at[row], raw.at[row, 0], load_sem.at[place, 0]),
                pltpu.make_async_copy(v_ref.at[row], raw.at[row, 1], load_sem.at[place, 1]),
                pltpu.make_async_copy(t_ref.at[row], raw.at[row, 2], load_sem.at[place, 2]),
            ]
        )
        for copy in loads[-1]:
            copy.start()
    table_load = pltpu.make_async_copy(table_ref, table, table_sem)
    table_load.start()

    def mask_row(place):
        row = order[place]
        for copy in loads[place]:
            copy.wait()
        ones = keep[row].astype(F32).astype(BF16)
        for field in range(3):
            for sample in range(batch):
                part = pl.ds(sample * levels, levels)
                masked[row, field, part, :] = raw[row, field, part, :] * ones

    def remote(src, dst, send, recv):
        return pltpu.make_async_remote_copy(
            src_ref=src,
            dst_ref=dst,
            send_sem=send,
            recv_sem=recv,
            device_id=partner,
            device_id_type=pl.DeviceIdType.MESH,
        )

    field_copies = []

    def pack_row(piece, place):
        row = order[place]
        if mid and piece == 0:
            away = pl.ds(pl.multiple_of(other * half_columns, half_columns), half_columns)
            here = pl.ds(0, half_columns)
        else:
            away = here = pl.ds(0, columns)
        ends = []
        for field in range(3):
            packed[piece, here, pl.ds(field * body, body)] = masked[row, field, away, pl.ds(0, body)]
            ends.append(masked[row, field, away, pl.ds(body, tail)])
        packed[piece, here, pl.ds(3 * body, 3 * tail)] = jnp.concatenate(ends, axis=1)
        return here

    def send_row(piece, place):
        here = pack_row(piece, place)
        if place == 0:
            pl.semaphore_wait(barrier, 1 + len(strides))
        copy = remote(
            packed.at[piece, here, :],
            arrived.at[piece, here, :],
            field_send.at[piece],
            field_recv.at[piece],
        )
        copy.start()
        field_copies.append([copy])

    def far_field(piece, field):
        bulk = arrived[piece, :, pl.ds(field * body, body)]
        end = arrived[piece, :, pl.ds(3 * body + field * tail, tail)]
        return jnp.concatenate([bulk, end], axis=1)

    early = min(mid + 1, mid + half)
    for place in range(early):
        mask_row(place)
        send_row(place, place)
    for place in range(early, len(order)):
        mask_row(place)

    ones_row = jnp.ones((8, span), BF16)
    zonal_mine[...] = jnp.zeros_like(zonal_mine)
    for row in range(bands):
        zonal_mine[pl.ds(row, 1), :] = nt_dot(ones_row, masked[row, 1])[0:1]
        counts = nt_dot(ones_row, keep[row].astype(F32).astype(BF16))[0:1]
        zonal_mine[pl.ds(slab + row, 1), :] = jnp.concatenate([counts] * batch, axis=1)
    zonal_copy = remote(zonal_mine, zonal_theirs, zonal_sem.at[0], zonal_sem.at[1])
    zonal_copy.start()
    for place in range(early, mid + half):
        send_row(place, place)

    if mid:
        here = pl.ds(pl.multiple_of(me * half_columns, half_columns), half_columns)
        for field in range(3):
            own = masked[half, field, here, :]
            doubled[field, pl.ds(0, half_columns), :] = own
            doubled[field, pl.ds(half_columns, half_columns), :] = own
    table_load.wait()

    row_index = lax.broadcasted_iota(jnp.int32, (padded_rows, 1), 0)
    left_lanes = lax.broadcasted_iota(jnp.int32, (1, columns), 1) < half_columns
    back_copies = []

    def transform(part, near, far):
        parity = (row_index + 1 + part * rows) % 2
        sign = (1 - 2 * parity).astype(F32)
        pieces = []
        for trig in range(2):
            wave = table[part, trig]
            pieces.append([nt_dot(wave, near(f)) + sign * nt_dot(wave, far(f)) for f in range(3)])
        (uc, vc, tc), (us, vs, ts) = pieces
        return norm_factor * (vc * tc + vs * ts), norm_factor * (uc * vc + us * vs)

    def process(piece):
        for copy in field_copies[piece]:
            copy.wait_recv()
        is_mid = mid and piece == 0
        if is_mid:
            arrived[piece, pl.ds(half_columns, half_columns), :] = arrived[
                piece, pl.ds(0, half_columns), :
            ]
            near = lambda f: doubled[f]
        else:
            row = my_rows[piece - mid]
            near = lambda f: masked[row, f]
        far = lambda f: far_field(piece, f)
        heat, moment = transform(other, near, far)
        if is_mid:
            given[piece, 0] = jnp.where(left_lanes, heat, moment).astype(BF16)
        else:
            given[piece, 0] = heat.astype(BF16)
            given[piece, 1] = moment.astype(BF16)
        sent = pl.ds(0, rows_sent)
        copies = [
            remote(
                given.at[piece, which, sent, :],
                returned.at[piece, which, sent, :],
                back_send.at[piece, which],
                back_recv.at[piece, which],
            )
            for which in range(1 if is_mid else 2)
        ]
        for copy in copies:
            copy.start()
        back_copies.append(copies)
        heat, moment = transform(me, near, far)
        own_ref[piece, 0] = heat[:rows]
        own_ref[piece, 1] = moment[:rows]

    def mean_copy(step):
        stride = strides[step]
        block = pl.ds(mine // stride * stride, stride)
        return pltpu.make_async_remote_copy(
            src_ref=gathered.at[block],
            dst_ref=gathered.at[block],
            send_sem=mean_send.at[step],
            recv_sem=mean_recv.at[step],
            device_id=place_of(across(stride)),
            device_id_type=pl.DeviceIdType.MESH,
        )

    mean_copies = [mean_copy(step) for step in range(len(strides))]

    def pass_means(first, last):
        for step in range(first, last):
            if step > 0:
                mean_copies[step - 1].wait_recv()
            mean_copies[step].start()

    def share_means():
        zonal_copy.wait_recv()
        total = zonal_mine[...] + zonal_theirs[...]
        mean_mine[...] = jnp.zeros_like(mean_mine)
        mean_mine[pl.ds(0, slab), :] = total[:slab] / jnp.maximum(total[slab:], 1.0)
        target = jnp.concatenate([target_ref[:, b, :] for b in range(batch)], axis=1)
        mean_mine[pl.ds(slab, bands), :] = target
        gathered[mine] = mean_mine[...]

    def finish_stream():
        mean_copies[-1].wait_recv()
        height = groups * slab
        cosine = cosine_ref[...]
        depth = jnp.concatenate([depth_ref[...]] * batch, axis=1)
        mean = gathered[:, 0:slab, :].reshape(height, columns)
        target = gathered[:, slab : 2 * slab, :].reshape(height, columns)
        stream = mean * cosine * depth
        lane = lax.broadcasted_iota(jnp.int32, (height, columns), 1) % levels
        line = lax.broadcasted_iota(jnp.int32, (height, columns), 0)
        step = 1
        while step < levels:
            stream = stream + jnp.where(lane >= step, pltpu.roll(stream, step, 1), 0.0)
            step *= 2
        step = 1
        while step < height:
            stream = stream + jnp.where(line >= step, pltpu.roll(stream, step, 0), 0.0)
            step *= 2
        peak = jnp.max(jnp.abs(stream))
        stream = stream / (peak + epsilon)
        misfit = jnp.sum(cosine * (stream - target) ** 2)
        penalty_ref[...] = jnp.full((1, 1), misfit / (columns * bands * groups), F32)
        stream_buf[...] = stream
        own = stream_buf[pl.ds(pl.multiple_of(mine * slab, slab), slab), :][:bands]
        for b in range(batch):
            psi_ref[:, b, :] = own[:, b * levels : (b + 1) * levels]

    pieces = mid + half
    early_steps = max(len(strides) - 1, 1)
    for piece in range(pieces):
        if piece == min(1, pieces - 1):
            share_means()
            pass_means(0, 1)
        process(piece)
        if piece == pieces - 2:
            pass_means(1, early_steps)
    if pieces < 2:
        pass_means(1, early_steps)
    pass_means(early_steps, len(strides))
    finish_stream()
    for copies in back_copies:
        for copy in copies:
            copy.wait_recv()
    for copies in field_copies + back_copies:
        for copy in copies:
            copy.wait_send()
    zonal_copy.wait_send()

    for copy in mean_copies:
        copy.wait_send()


def assemble(sizes, psi_in, own_ref, returned, penalty_in, psi_ref, heat_ref, moment_ref, penalty_ref, stage, sems):
    bands, batch, levels, rows = sizes
    columns = batch * levels
    half, mid = bands // 2, bands % 2
    half_columns = columns // 2
    me = lax.axis_index("lon")
    other = 1 - me
    copies = []

    def put(row, slot, heat, moment):
        stage[slot, 0] = heat
        stage[slot, 1] = moment
        for which, out in enumerate((heat_ref, moment_ref)):
            copy = pltpu.make_async_copy(stage.at[slot, which], out.at[row], sems.at[slot, which])
            copy.start()
            copies.append(copy)

    for i in range(half):
        piece = mid + i
        for which, out in enumerate((heat_ref, moment_ref)):
            copy = pltpu.make_async_copy(
                own_ref.at[piece, which], out.at[me * (half + mid) + i], sems.at[half + mid + i, which]
            )
            copy.start()
            copies.append(copy)
    for i in range(half):
        piece = mid + i
        put(
            other * (half + mid) + i,
            piece,
            returned[piece, 0, :rows].astype(F32),
            returned[piece, 1, :rows].astype(F32),
        )
    if mid:
        both = returned[0, 0, :rows].astype(F32)
        turned = pltpu.roll(both, half_columns, 1)
        mine_lanes = (lax.broadcasted_iota(jnp.int32, (1, columns), 1) // half_columns) == me
        first = me == 0
        put(
            half,
            0,
            jnp.where(mine_lanes, own_ref[0, 0], jnp.where(first, turned, both)),
            jnp.where(mine_lanes, own_ref[0, 1], jnp.where(first, both, turned)),
        )
    psi_ref[...] = psi_in[...]
    penalty_ref[...] = penalty_in[...]
    for copy in copies:
        copy.wait()


def per_device(mesh_shape, u, v, t, keep, depth, target):
    bands, batch, levels, span = v.shape
    lon_ways = mesh_shape["lon"]
    assert lon_ways == 2
    lev_ways = mesh_shape["lev"]
    groups = mesh_shape["lat"] * lev_ways
    assert groups > 1 and groups & (groups - 1) == 0
    rows = HARMONIC_ORDERS // lon_ways
    padded = round_up(rows, 128)
    rows_sent = round_up(rows, 16)
    columns = batch * levels
    half, mid = bands // 2, bands % 2
    pieces = half + mid
    slab = round_up(bands, 8)
    nlat = bands * groups
    table = jnp.asarray(wave_table(span * lon_ways, lon_ways, rows, padded, span))
    latitude = ((np.arange(nlat).astype(np.float32) + np.float32(0.5)) / np.float32(nlat) - np.float32(0.5)) * np.float32(math.pi)
    cosine = np.zeros((groups, slab, 1), np.float32)
    cosine[:, :bands, 0] = np.cos(latitude).reshape(groups, bands)
    cosine = jnp.asarray(np.broadcast_to(cosine.reshape(groups * slab, 1), (groups * slab, columns)).copy())
    fields = [x.reshape(bands, columns, span) for x in (u, v, t)]
    sizes = (bands, batch, levels, span, rows, rows_sent, groups, lev_ways)
    anywhere = pl.BlockSpec(memory_space=pl.ANY)
    inside = pl.BlockSpec(memory_space=pltpu.VMEM)
    in_hbm = pl.BlockSpec(memory_space=pltpu.MemorySpace.HBM)
    body = span // 128 * 128
    lanes = 3 * body + round_up(3 * (span - body), 128)
    mid_results = pl.pallas_call(
        functools.partial(kernel, sizes),
        out_shape=(
            pltpu.MemorySpace.VMEM((bands, batch, levels), F32),
            pltpu.MemorySpace.VMEM((pieces, 2, rows, columns), F32),
            pltpu.MemorySpace.VMEM((pieces, 2, padded, columns), BF16),
            pltpu.MemorySpace.VMEM((1, 1), F32),
        ),
        in_specs=[in_hbm] * 5 + [inside] * 3,
        out_specs=(inside,) * 4,
        scratch_shapes=[
            pltpu.VMEM((bands, 3, columns, span), BF16),
            pltpu.VMEM((bands, levels, span), jnp.int32),
            pltpu.VMEM((bands, 3, columns, span), BF16),
            pltpu.VMEM((3, columns, span), BF16),
            pltpu.VMEM((pieces, columns, lanes), BF16),
            pltpu.VMEM((pieces, columns, lanes), BF16),
            pltpu.VMEM(table.shape, BF16),
            pltpu.VMEM((pieces, 2, padded, columns), BF16),
            pltpu.VMEM((2 * slab, columns), F32),
            pltpu.VMEM((2 * slab, columns), F32),
            pltpu.VMEM((2 * slab, columns), F32),
            pltpu.VMEM((groups, 2 * slab, columns), F32),
            pltpu.VMEM((groups * slab, columns), F32),
            pltpu.SemaphoreType.DMA((bands, 4)),
            pltpu.SemaphoreType.DMA,
            pltpu.SemaphoreType.DMA((pieces,)),
            pltpu.SemaphoreType.DMA((pieces,)),
            pltpu.SemaphoreType.DMA((pieces, 2)),
            pltpu.SemaphoreType.DMA((pieces, 2)),
            pltpu.SemaphoreType.DMA((2,)),
            pltpu.SemaphoreType.DMA((groups,)),
            pltpu.SemaphoreType.DMA((groups,)),
        ],
        compiler_params=pltpu.CompilerParams(
            collective_id=0, has_side_effects=True, vmem_limit_bytes=56 * 1024 * 1024
        ),
    )(*fields, keep, table, cosine, depth.reshape(1, levels), target)
    psi, heat, moment, penalty = pl.pallas_call(
        functools.partial(assemble, (bands, batch, levels, rows)),
        out_shape=(
            jax.ShapeDtypeStruct((bands, batch, levels), F32),
            jax.ShapeDtypeStruct((bands, rows, columns), F32),
            jax.ShapeDtypeStruct((bands, rows, columns), F32),
            jax.ShapeDtypeStruct((1, 1), F32),
        ),
        in_specs=[inside] * 4,
        out_specs=(inside, anywhere, anywhere, inside),
        scratch_shapes=[
            pltpu.VMEM((pieces, 2, rows, columns), F32),
            pltpu.SemaphoreType.DMA((pieces + half, 2)),
        ],
        compiler_params=pltpu.CompilerParams(vmem_limit_bytes=8 * 1024 * 1024),
    )(*mid_results)
    return psi, heat.transpose(1, 0, 2), moment.transpose(1, 0, 2), penalty.reshape(())


def solution(mesh):
    banded = ("lat", "lev")
    placed = (
        P(banded, None, None, "lon"),
        P(banded, None, None, "lon"),
        P(banded, None, None, "lon"),
        P(banded, None, "lon"),
        P(),
        P(banded, None, None),
    )
    return jax.shard_map(
        functools.partial(per_device, dict(mesh.shape)),
        mesh=mesh,
        in_specs=placed,
        out_specs=(P(banded, None, None), P("lon", banded, None), P("lon", banded, None), P()),
        check_vma=False,
    )
```
